32 devices in a mesh: expert: 4 (over y, x), ffn: 8 (over z, core).
Axes of the slice: x: 2, y: 2, z: 4, core: 2. Of those that a mesh axis runs over, the one named last changes fastest.
Arguments:
- tokens: bfloat16 [1024, 4096], P('expert'), may hold values from -6 to 6
- router_gates: float32 [1024, 2], P('expert'), may hold values from 0.1 to 1
- routes: int32 [1024, 2], P('expert'), may hold values from 0 to 3, all different within a row; in each aligned block of 256 rows (0 to 255, 256 to 511, ...) at most 256 rows name the same one
- gate_proj: bfloat16 [4, 4096, 14336], P('expert', None, 'ffn'), may hold values from -0.09375 to 0.09375
- up_proj: bfloat16 [4, 4096, 14336], P('expert', None, 'ffn'), may hold values from -0.09375 to 0.09375
- down_proj: bfloat16 [4, 14336, 4096], P('expert', 'ffn'), may hold values from -0.0625 to 0.0625
Outputs:
- mixed: bfloat16 [1024, 4096], P('expert', 'ffn')
The draws below stay inside these ranges and needn't reach their ends.
Inputs may be any that keep to these rules, and one draw needn't show every extreme that they name: `routes`: the 2 experts of a token differ. Among the tokens of one index of the expert axis (aligned blocks of 256 tokens) no expert is chosen by more than 256 tokens, and in some blocks one expert is chosen by exactly 256.
All inputs are finite; a program needn't handle non-finite values.
Results may differ from the reference program's by a relative error of at most 0.017.
Values may be sent and summed in bfloat16 or wider, within the bound.
A program may use at most 128 MiB of HBM per device.

```python
import math
import jax
import jax.numpy as jnp
import numpy as np
from jax import lax

D = 4096
FF = 14336
TOP = 2
TOK_DEV = 256
EXPERTS = 4
CAP = 256
TOKENS = 1024
N_FFN = 8


def strengthened(values, rng, source, target, parts, factor):
    def block_of(dim):
        return (jnp.arange(values.shape[dim]) // (values.shape[dim] // parts)).reshape((-1,) + (1,) * (values.ndim - 1 - dim))

    one_side = jax.random.permutation(rng, parts)[block_of(target)]
    other_side = (block_of(target) + parts // 2) % parts
    return jnp.where((block_of(source) == one_side) | (block_of(source) == other_side), factor * values, values)


def steps_of(key, dims, pieces, low, high):
    loudness = 1.0
    for axis_at, shards_of in pieces:
        steps = jax.random.uniform(jax.random.fold_in(jax.random.fold_in(key, 6), axis_at), (shards_of,), jnp.float32, low / len(pieces), high / len(pieces))
        loudness = loudness * jnp.repeat(jnp.exp(steps), dims[axis_at] // shards_of).reshape((-1,) + (1,) * (len(dims) - 1 - axis_at))
    return loudness


def shared_out(key, own, number, rows, count, top, limit, lean):
    sequence = jax.random.permutation(key, count)
    crowded, ordinary = load_shares(count, rows * top, limit, lean, True), load_shares(count, rows * top, limit, lean, False)
    places = jnp.arange(count)

    def named(lengths, offset_by):
        used = int((lengths > 0).sum())
        fixed = max(1, used // 4)
        passed = fixed + (places - fixed + offset_by * (used - fixed)) % max(1, count - fixed)
        return jnp.zeros((count,), jnp.int32).at[sequence[jnp.where(places < fixed, places, passed)]].set(jnp.asarray(lengths, jnp.int32))

    lengths = jnp.where(number % 4 == 0, named(crowded, number // 4), named(ordinary, number - number // 4 - 1))
    mixed = jax.random.permutation(jax.random.fold_in(own, 3), count)
    source_of, taker = mixed[0:count // 2 * 2:2], mixed[1:count // 2 * 2:2]
    slack = jnp.minimum(lengths[source_of] - 1, limit - lengths[taker]) // 2
    slack = jnp.where((source_of == sequence[0]) | (taker == sequence[0]) | (lengths[taker] == 0), 0, jnp.maximum(slack, 0))
    passed = jax.random.randint(jax.random.fold_in(own, 4), (count // 2,), 0, 1 << 20) % (slack + 1)
    lengths = lengths.at[source_of].add(-passed).at[taker].add(passed)
    labels = jnp.searchsorted(jnp.cumsum(lengths), jnp.arange(rows * top), side="right").astype(jnp.int32)
    grid = labels.reshape(top, rows).T
    grid = grid[jax.random.permutation(jax.random.fold_in(own, 1), rows)]
    offset_by = jax.random.randint(jax.random.fold_in(own, 2), (rows, 1), 0, top)
    return jnp.take_along_axis(grid, (jnp.arange(top)[None, :] + offset_by) % top, axis=1)


def load_shares(number_of, total, reach, lean, full):
    weights = [(1 << 20) // math.isqrt(standing ** lean) + 1 for standing in range(1, number_of + 1)]
    largest = reach if full else min(reach, max(-(-total // number_of), total * weights[0] // sum(weights)))
    least = 1 if total - largest >= number_of - 1 else 0
    holding, surplus = [largest] + [least] * (number_of - 1), total - largest - least * (number_of - 1)
    while surplus > 0:
        free = [i for i in range(1, number_of) if holding[i] < largest] or [i for i in range(1, number_of) if holding[i] < reach]
        pool, budget = sum([weights[i] for i in free]), surplus
        for i in free:
            extra = min(reach - holding[i], max(1, budget * weights[i] // pool), surplus)
            holding[i] = holding[i] + extra
            surplus = surplus - extra
    return np.array(holding)


def centred(own_key, shape, deviation, most, shards=(), kind=jnp.bfloat16):
    entries = deviation * jax.random.normal(own_key, shape, jnp.float32)
    if shards:
        entries = entries * steps_of(own_key, shape, shards, -0.22, 0.18)
    return jnp.clip(entries, -most, most).astype(kind)


def gaussian_with(own_key, extent, spread, bound, cuts, heavy, kind=jnp.bfloat16):
    drawn = spread * jax.random.normal(own_key, extent, jnp.float32)
    if cuts:
        drawn = drawn * steps_of(own_key, extent, cuts, -0.22, 0.18)
    return jnp.clip(strengthened(drawn, jax.random.fold_in(own_key, 3), *heavy), -bound, bound).astype(kind)


def setup_inputs(seed: int = 0) -> dict:
    streams_of = jax.random.split(jax.random.key(seed), 7)
    tokens = centred(streams_of[0], (TOKENS, D), 1.0, 6.0, ((0, 4),))
    router_gates = jnp.clip(jnp.exp(math.log(1.0) - 2.3025851 * jax.random.uniform(streams_of[1], (TOKENS, TOP), jnp.float32) ** steps_of(streams_of[1], (TOKENS, TOP), ((0, 4),), -0.2, 0.2)), 0.1, 1.0)
    routes_keys = jax.random.split(jax.random.fold_in(streams_of[2], 1), TOKENS // TOK_DEV)
    routes_turns = jax.random.permutation(jax.random.fold_in(streams_of[2], 3), TOKENS // TOK_DEV)
    routes = jax.vmap(lambda own, number: shared_out(jax.random.fold_in(streams_of[2], 2), own, number, TOK_DEV, EXPERTS, TOP, CAP, 2))(routes_keys, routes_turns).reshape((TOKENS, TOP))
    gate_proj = centred(streams_of[3], (EXPERTS, D, FF), D ** -0.5, 0.09375, ((0, 4), (2, 8)))
    up_proj = centred(streams_of[4], (EXPERTS, D, FF), D ** -0.5, 0.09375, ((0, 4), (2, 8)))
    down_proj = gaussian_with(streams_of[5], (EXPERTS, FF, D), FF ** -0.5, 0.0625, ((0, 4), (1, 8)), (1, 2, 8, 2.0))
    return {"tokens": tokens, "router_gates": router_gates, "routes": routes, "gate_proj": gate_proj, "up_proj": up_proj, "down_proj": down_proj}


def slot_numbers(routes):
    grouped = routes.reshape(-1, TOK_DEV * TOP)
    chosen = (grouped[:, :, None] == jnp.arange(EXPERTS, dtype=jnp.int32)[None, None, :]).astype(jnp.int32)
    ranking = jnp.cumsum(chosen, axis=1) - chosen
    return jnp.sum(ranking * chosen, axis=2).reshape(-1, TOP).astype(jnp.int32)


def run_expert(operands):
    buffer_rows, gate_matrix, up_matrix, down_matrix = operands
    gate_act = jnp.dot(buffer_rows, gate_matrix, preferred_element_type=jnp.float32)
    up_act = jnp.dot(buffer_rows, up_matrix, preferred_element_type=jnp.float32)
    hidden = (jax.nn.silu(gate_act) * up_act).astype(jnp.bfloat16)
    shard_width = FF // N_FFN

    def add_shard(running, shard_index):
        hidden_part = lax.dynamic_slice_in_dim(hidden, shard_index * shard_width, shard_width, 1)
        down_part = lax.dynamic_slice_in_dim(down_matrix, shard_index * shard_width, shard_width, 0)
        rounded = jnp.dot(hidden_part, down_part, preferred_element_type=jnp.float32).astype(jnp.bfloat16)
        rounded = lax.optimization_barrier(rounded)
        return running + rounded.astype(jnp.float32), None

    start_sum = jnp.zeros((buffer_rows.shape[0], D), jnp.float32)
    result, unused = lax.scan(add_shard, start_sum, jnp.arange(N_FFN, dtype=jnp.int32))
    return result


def reference(tokens, router_gates, routes, gate_proj, up_proj, down_proj):
    sources = TOKENS // TOK_DEV
    slot = slot_numbers(routes)
    owner = (jnp.arange(TOKENS, dtype=jnp.int32) // TOK_DEV)[:, None]
    position = (owner * CAP + slot).astype(jnp.int32)
    buffers = jnp.zeros((EXPERTS, sources * CAP, D), jnp.bfloat16)
    buffers = buffers.at[routes, position].set(jnp.broadcast_to(tokens[:, None, :], (TOKENS, TOP, D)))
    outputs = lax.map(run_expert, (buffers, gate_proj, up_proj, down_proj))
    picked = outputs[routes, position]
    mixed = jnp.sum(router_gates[:, :, None] * picked, axis=1)
    return mixed.astype(jnp.bfloat16)
```

```python
import functools

import jax
import jax.numpy as jnp
from jax import lax
from jax.experimental import pallas as pl
from jax.experimental.pallas import tpu as pltpu
from jax.sharding import PartitionSpec as P

MESH = pl.DeviceIdType.MESH
VMEM_BYTES = 67043328


def flip(index, mask, size):
    result, bit = 0, 1
    while bit < size:
        digit = (index // bit) % 2
        result = result + bit * ((1 - digit) if mask & bit else digit)
        bit *= 2
    return result


def layer_kernel(
    experts, groups, tile, out_tile,
    tokens_hbm, gates_ref, routes_ref, gate_hbm, up_hbm, down_hbm,
    out_ref,
    gate, up, down, blk, hid, part, pair, returned, *rest,
):
    stages = groups.bit_length() - 2
    stage_in, rest = rest[:stages], rest[stages:]
    (gate_sem, up_sem, down_sem, own_sem, tok_s, tok_r, fwd_s, fwd_r, diag_s, diag_r,
     pair_s, pair_r, stage_s, stage_r, ret_s, ret_r) = rest
    rows, width = blk.shape[1], blk.shape[2]
    hidden = gate.shape[1]
    half, quarter = rows // 2, rows // 4
    eighth = quarter // 2
    cols = width // groups
    count = groups // 2
    tiles, out_tiles = hidden // tile, width // out_tile
    per_tile = out_tile // cols
    e, f = lax.axis_index("expert"), lax.axis_index("ffn")
    core = f % 2
    near = {k: (flip(e, k, experts), f) for k in range(1, experts)}
    mates = [(e, flip(f, 1 << s, groups)) for s in range(stages + 1)]

    barrier = pltpu.get_barrier_semaphore()
    partners = list(near.values()) + mates
    for partner in partners:
        pl.semaphore_signal(barrier, inc=1, device_id=partner, device_id_type=MESH)

    def gate_copy(j):
        s = pl.ds(j * tile, tile)
        return pltpu.make_async_copy(gate_hbm.at[:, s], gate.at[:, s], gate_sem.at[j])

    def up_copy(j):
        s = pl.ds(j * tile, tile)
        return pltpu.make_async_copy(up_hbm.at[:, s], up.at[:, s], up_sem.at[j])

    def down_copy(n):
        s = pl.ds(n * out_tile, out_tile)
        return pltpu.make_async_copy(down_hbm.at[:, s], down.at[:, s], down_sem.at[n])

    own_copy = pltpu.make_async_copy(tokens_hbm, blk.at[0], own_sem)
    own_copy.start()
    for j in range(tiles):
        gate_copy(j).start()
        up_copy(j).start()
    for n in range(out_tiles):
        down_copy(n).start()

    def place(k, h):
        return (1 + h, (k - 1) * half) if k < 3 else (k, h * half)

    def remote(src, dst, ss, rs, device):
        return pltpu.make_async_remote_copy(
            src_ref=src, dst_ref=dst, send_sem=ss, recv_sem=rs, device_id=device, device_id_type=MESH
        )

    def spot(k, h):
        b, row = place(k, h)
        return blk.at[b, pl.ds(pl.multiple_of(row + core * quarter, quarter), quarter)]

    def token_copy(k, h):
        row = pl.multiple_of(h * half + core * quarter, quarter)
        return remote(tokens_hbm.at[pl.ds(row, quarter)], spot(k, h), tok_s.at[k, h], tok_r.at[k, h], near[k])

    def forward_copy(k, h):
        return remote(spot(k, h), spot(k, h), fwd_s.at[k, h], fwd_r.at[k, h], mates[0])

    def diag_copy(i, h):
        source, offset = (2, 0) if i == 0 else (1, eighth)
        b, row = place(source, h)
        src = blk.at[b, pl.ds(pl.multiple_of(row + core * quarter + offset, eighth), eighth)]
        b, row = place(3, h)
        dst = blk.at[b, pl.ds(pl.multiple_of(row + core * quarter + offset, eighth), eighth)]
        return remote(src, dst, diag_s.at[i, h], diag_r.at[i, h], near[1 + i])

    pl.semaphore_wait(barrier, len(partners))
    direct = [k for k in range(1, experts) if k != 3]
    for h in range(2):
        for k in (1, 2):
            token_copy(k, h).start()
    for k in direct[2:]:
        for h in range(2):
            token_copy(k, h).start()

    def pass_on(h):
        for k in (1, 2):
            token_copy(k, h).wait_recv()
            forward_copy(k, h).start()
        for i in range(2):
            diag_copy(i, h).start()

    def prepare(b):
        if b < 3:
            pass_on(b - 1)
        elif b == 3:
            for h in range(2):
                for i in range(2):
                    diag_copy(i, h).wait_recv()
                forward_copy(3, h).start()
        else:
            for h in range(2):
                token_copy(b, h).wait_recv()
                forward_copy(b, h).start()

    def arrive(b):
        pairs = [(1, b - 1), (2, b - 1)] if b < 3 else [(b, 0), (b, 1)]
        for k, h in pairs:
            forward_copy(k, h).wait_recv()

    def pair_copy(b, n):
        return remote(part.at[1, n], pair.at[b, n], pair_s.at[b, n], pair_r.at[b, n], mates[0])

    def kept(stage, m):
        index, low = 0, 1
        for s in range(1, stage + 1):
            index = index + low * ((f // (1 << s)) % 2)
            low *= 2
        return index + low * m

    def stage_copy(stage, b, m):
        low = 1 << (stage - 1)
        digit = (f // (1 << stage)) % 2
        base = kept(stage - 1, 0)
        src = pair.at[b, base + low * (1 - digit) + 2 * low * m]
        return remote(
            src, stage_in[stage - 1].at[b, m],
            stage_s.at[stage - 1, b, m], stage_r.at[stage - 1, b, m], mates[stage],
        )

    def pieces(stage):
        return count >> stage

    def join_pair(b):
        for n in range(count):
            pair_copy(b, n).wait()
            pair[b, n] = (part[0, n].astype(jnp.float32) + pair[b, n].astype(jnp.float32)).astype(pair.dtype)
        for m in range(pieces(1)):
            stage_copy(1, b, m).start()

    def join_stage(stage, b):
        for m in range(pieces(stage)):
            stage_copy(stage, b, m).wait()
            at = kept(stage, m)
            got = stage_in[stage - 1][b, m].astype(jnp.float32)
            pair[b, at] = (pair[b, at].astype(jnp.float32) + got).astype(pair.dtype)
        if stage < stages:
            for m in range(pieces(stage + 1)):
                stage_copy(stage + 1, b, m).start()

    def return_copy(b, j):
        k, h = (j + 1, b - 1) if b < 3 else (b, j)
        src = pair.at[b, f // 2, pl.ds(j * half, half)]
        return remote(
            src, returned.at[k - 1, pl.ds(h * half, half)], ret_s.at[k, h], ret_r.at[k, h], near[k]
        )

    def give_back(b):
        if b > 0:
            for j in range(2):
                return_copy(b, j).start()

    def compute(b, first, hooks):
        for j in range(tiles):
            if first:
                if j == 0:
                    own_copy.wait()
                gate_copy(j).wait()
                up_copy(j).wait()
            s = pl.ds(j * tile, tile)
            gate_act = jnp.dot(blk[b], gate[:, s], preferred_element_type=jnp.float32)
            up_act = jnp.dot(blk[b], up[:, s], preferred_element_type=jnp.float32)
            hid[:, s] = (gate_act / (1.0 + jnp.exp(-gate_act)) * up_act).astype(hid.dtype)
            hooks(("mid", j))
        for n in range(out_tiles):
            if first:
                down_copy(n).wait()
            s = pl.ds(n * out_tile, out_tile)
            acc = jnp.dot(hid[...], down[:, s], preferred_element_type=jnp.float32).astype(part.dtype)
            for i in range(per_tile):
                block = n * per_tile + i
                part[(block + core) % 2, block // 2] = acc[:, i * cols : (i + 1) * cols]
            for m in range(n * per_tile // 2, (n + 1) * per_tile // 2):
                pair_copy(b, m).start()
            hooks(("end", n))

    def first_hooks(at):
        if at == ("end", out_tiles // 2 - 1):
            prepare(1)

    compute(0, True, first_hooks)

    @pl.loop(1, experts)
    def _(step):
        for b in range(1, experts):
            @pl.when(step == b)
            def _():
                arrive(b)

        def hooks(at):
            if at == ("mid", 0):
                join_pair(step - 1)
            if at == ("mid", 1):
                @pl.when(step >= 2)
                def _():
                    join_stage(1, step - 2)
            if at == ("mid", tiles - 1):
                for b in range(1, experts - 1):
                    @pl.when(step == b)
                    def _():
                        prepare(b + 1)

        compute(step, False, hooks)

    join_pair(experts - 1)
    for b in range(experts - 2):
        for stage in range(2, stages + 1):
            join_stage(stage, b)
        give_back(b)
    for b in range(experts - 2, experts):
        join_stage(1, b)
    for b in range(experts - 2, experts):
        for stage in range(2, stages + 1):
            join_stage(stage, b)
        give_back(b)

    for k in range(1, experts):
        for h in range(2):
            if k != 3:
                token_copy(k, h).wait_send()
            forward_copy(k, h).wait_send()
    for i in range(2):
        for h in range(2):
            diag_copy(i, h).wait_send()

    def weight_of(k):
        name = flip(e, k, experts)
        total = jnp.zeros((rows, 1), jnp.float32)
        for t in range(routes_ref.shape[1]):
            total = total + jnp.where(routes_ref[:, t : t + 1] == name, gates_ref[:, t : t + 1], 0.0)
        return total

    result = weight_of(0) * pair[0, f // 2].astype(jnp.float32)
    for b in range(1, experts):
        for j in range(2):
            return_copy(b, j).wait()
    for k in range(1, experts):
        result = result + weight_of(k) * returned[k - 1].astype(jnp.float32)
    out_ref[...] = result.astype(out_ref.dtype)


def per_device(experts, groups, tokens, router_gates, routes, gate_proj, up_proj, down_proj):
    rows, width = tokens.shape
    hidden = gate_proj.shape[2]
    cols = width // groups
    count = groups // 2
    stages = groups.bit_length() - 2
    tile = 256 if hidden % 256 == 0 else 128
    out_tile = 1024
    bf16 = jnp.bfloat16
    dma = pltpu.SemaphoreType.DMA
    vmem = pl.BlockSpec(memory_space=pltpu.VMEM)
    hbm = pl.BlockSpec(memory_space=pl.ANY)
    scratch = [
        pltpu.VMEM((width, hidden), bf16),
        pltpu.VMEM((width, hidden), bf16),
        pltpu.VMEM((hidden, width), bf16),
        pltpu.VMEM((experts, rows, width), bf16),
        pltpu.VMEM((rows, hidden), bf16),
        pltpu.VMEM((2, count, rows, cols), bf16),
        pltpu.VMEM((experts, count, rows, cols), bf16),
        pltpu.VMEM((experts - 1, rows, cols), bf16),
    ]
    scratch += [pltpu.VMEM((experts, count >> s, rows, cols), bf16) for s in range(1, stages + 1)]
    scratch += [
        dma((hidden // tile,)), dma((hidden // tile,)), dma((width // out_tile,)), dma,
        dma((experts, 2)), dma((experts, 2)), dma((experts, 2)), dma((experts, 2)),
        dma((2, 2)), dma((2, 2)),
        dma((experts, count)), dma((experts, count)),
        dma((stages, experts, count // 2)), dma((stages, experts, count // 2)),
        dma((experts, 2)), dma((experts, 2)),
    ]
    return pl.pallas_call(
        functools.partial(layer_kernel, experts, groups, tile, out_tile),
        name="layer",
        out_shape=jax.ShapeDtypeStruct((rows, cols), bf16),
        in_specs=[hbm, vmem, vmem, hbm, hbm, hbm],
        out_specs=vmem,
        scratch_shapes=scratch,
        compiler_params=pltpu.CompilerParams(
            collective_id=0, has_side_effects=True, vmem_limit_bytes=VMEM_BYTES
        ),
    )(tokens, router_gates, routes, gate_proj[0], up_proj[0], down_proj[0])


def solution(mesh):
    in_specs = (
        P("expert", None),
        P("expert", None),
        P("expert", None),
        P("expert", None, "ffn"),
        P("expert", None, "ffn"),
        P("expert", "ffn", None),
    )
    body = functools.partial(per_device, mesh.shape["expert"], mesh.shape["ffn"])
    return jax.shard_map(
        body, mesh=mesh, in_specs=in_specs, out_specs=P("expert", "ffn"), check_vma=False
    )
```

```python
import functools

import jax
import jax.numpy as jnp
from jax import lax
from jax.experimental import pallas as pl
from jax.experimental.pallas import tpu as pltpu
from jax.sharding import PartitionSpec as P

MESH = pl.DeviceIdType.MESH
VMEM_BYTES = 67043328
AHEAD = 3


def flip(index, mask, size):
    result, bit = 0, 1
    while bit < size:
        digit = (index // bit) % 2
        result = result + bit * ((1 - digit) if mask & bit else digit)
        bit *= 2
    return result


def layer_kernel(
    experts, groups, tile,
    tokens_hbm, gates_ref, routes_ref, gate_hbm, up_hbm, down_hbm,
    out_ref,
    gate, up, down, blk, hid, part, pair, returned, table, their_gates, their_routes, their_table,
    *rest,
):
    stages = groups.bit_length() - 2
    sum_in, far_in, rest = rest[:stages], rest[stages : 2 * stages], rest[2 * stages :]
    (weight_sem, own_sem, tok_s, tok_r, fwd_s, fwd_r, relay_s, relay_r,
     pair_s, pair_r, met_s, met_r, stage_s, stage_r, ret_s, ret_r,
     detour_s, detour_r, route_s, route_r) = rest
    rows, width = blk.shape[1], blk.shape[2]
    hidden = gate.shape[1]
    half, quarter, piece = rows // 2, rows // 4, rows // 8
    cols = width // groups
    count = groups // 2
    tiles, out_tile = hidden // tile, 2 * cols
    last = experts - 1
    e, f = lax.axis_index("expert"), lax.axis_index("ffn")
    core = f % 2
    near = {k: (flip(e, k, experts), f) for k in range(1, experts)}
    mates = [(e, flip(f, 1 << s, groups)) for s in range(stages + 1)]
    far = list(range(3, experts))
    f32 = jnp.float32

    barrier = pltpu.get_barrier_semaphore()
    partners = list(near.values()) + mates
    for partner in partners:
        pl.semaphore_signal(barrier, inc=1, device_id=partner, device_id_type=MESH)

    own_copy = pltpu.make_async_copy(tokens_hbm, blk.at[0], own_sem)

    def columns(t):
        index = 0
        for s in range(1, stages + 1):
            digit = (f // (1 << s)) % 2
            index = index + (1 << (s - 1)) * (digit if (t >> (stages - s)) & 1 else 1 - digit)
        return pl.ds(pl.multiple_of(index * out_tile, out_tile), out_tile)

    def weight_group(i):
        if i < tiles:
            s = pl.ds(i * tile, tile)
            return [
                pltpu.make_async_copy(gate_hbm.at[:, s], gate.at[:, s], weight_sem.at[0, i]),
                pltpu.make_async_copy(up_hbm.at[:, s], up.at[:, s], weight_sem.at[1, i]),
            ]
        s = columns(i - tiles)
        return [pltpu.make_async_copy(down_hbm.at[:, s], down.at[:, s], weight_sem.at[0, i])]

    def start_weights(i):
        if i < tiles + count:
            for copy in weight_group(i):
                copy.start()

    def take_weights(i):
        for copy in weight_group(i):
            copy.wait()
        start_weights(i + AHEAD)

    own_copy.start()
    for i in range(AHEAD):
        start_weights(i)

    def place(k, h):
        return (last if h else 1, (k - 1) * half) if k < 3 else (k - 1, h * half)

    def remote(src, dst, ss, rs, device):
        return pltpu.make_async_remote_copy(
            src_ref=src, dst_ref=dst, send_sem=ss, recv_sem=rs, device_id=device, device_id_type=MESH
        )

    def spot(k, h, i):
        b, row = place(k, h)
        return blk.at[b, pl.ds(pl.multiple_of(row + core * quarter + i * piece, piece), piece)]

    def token_copy(k, h, i):
        row = pl.multiple_of(h * half + core * quarter + i * piece, piece)
        return remote(
            tokens_hbm.at[pl.ds(row, piece)], spot(k, h, i), tok_s.at[k, h, i], tok_r.at[k, h, i], near[k]
        )

    def forward_copy(k, h, i):
        return remote(spot(k, h, i), spot(k, h, i), fwd_s.at[k, h, i], fwd_r.at[k, h, i], mates[0])

    def weight_rows(gates, routes, name):
        total = jnp.zeros((1, rows), f32)
        for t in range(routes.shape[0]):
            total = total + jnp.where(routes[t : t + 1, :] == name, gates[t : t + 1, :], 0.0)
        return jnp.broadcast_to(total, (128, rows)).T

    def route_copies(k):
        return [
            remote(ref, theirs.at[k - 1], route_s.at[i, k - 1], route_r.at[i, k - 1], near[k])
            for i, (ref, theirs) in enumerate([(gates_ref, their_gates), (routes_ref, their_routes)])
        ]

    def relay_copy(i):
        return remote(spot(2 - i, 0, i), spot(3, 0, i), relay_s.at[i], relay_r.at[i], near[1 + i])

    for k in range(experts):
        table[k] = weight_rows(gates_ref[...], routes_ref[...], flip(e, k, experts))
    pl.semaphore_wait(barrier, len(partners))
    for i in range(2):
        for k in (1, 2):
            token_copy(k, 0, i).start()
    for k in (1, 2):
        for copy in route_copies(k):
            copy.start()
    for k in far:
        for h in range(1 if k == 3 else 0, 2):
            for i in range(2):
                token_copy(k, h, i).start()

    def pass_first(i):
        for k in (1, 2):
            token_copy(k, 0, i).wait_recv()
            forward_copy(k, 0, i).start()
        relay_copy(i).start()

    def send_second():
        for i in range(2):
            for k in (1, 2):
                token_copy(k, 1, i).start()

    def pass_second():
        for i in range(2):
            for k in (1, 2):
                token_copy(k, 1, i).wait_recv()
                forward_copy(k, 1, i).start()

    def pass_far(k):
        for h in (1, 0):
            for i in range(2):
                if k == 3 and h == 0:
                    relay_copy(i).wait_recv()
                else:
                    token_copy(k, h, i).wait_recv()
                forward_copy(k, h, i).start()

    def arrive(b):
        if b in (1, last):
            pairs = [(1, b // last), (2, b // last)]
        else:
            pairs = [(b + 1, 0), (b + 1, 1)]
        for k, h in pairs:
            for i in range(2):
                forward_copy(k, h, i).wait_recv()

    def pair_copy(b, n):
        return remote(part.at[1, n], pair.at[b, n], pair_s.at[b, n], pair_r.at[b, n], mates[0])

    def join_pair(b, n):
        pair_copy(b, n).wait()
        pair[b, n] = (part[0, n].astype(f32) + pair[b, n].astype(f32)).astype(pair.dtype)

    def met_copy(k, n):
        b, row = place(k, 1)
        return remote(
            pair.at[b, n, pl.ds(row, half)], met(k, n), met_s.at[k - 1, n], met_r.at[k - 1, n], near[k]
        )

    def hand_over(n):
        join_pair(last, n)
        add_detour(n)
        for k in (1, 2):
            met_copy(k, n).start()

    def weight_of(k, h):
        return table[k, pl.ds(h * half, half), 0:1]

    def learn_routes():
        for k in (1, 2):
            for copy in route_copies(k):
                copy.wait_recv()
            for i, name in enumerate([e, near[3 - k][0]]):
                their_table[k - 1, i] = weight_rows(their_gates[k - 1], their_routes[k - 1], name)[half:]

    def met(k, n):
        return blk.at[0, pl.ds((k - 1) * half, half), pl.ds(n * cols, cols)]

    def detour(k, n):
        return blk.at[0, pl.ds((k - 1) * quarter, quarter), pl.ds(width // 2 + n * cols, cols)]

    def home(k):
        if k < 4:
            return blk.at[0, pl.ds(half, half), pl.ds(width // 2 + (k - 1) * cols, cols)]
        return returned.at[k - 4]

    def detour_copy(k, n):
        src = pair.at[2, n, pl.ds(half + (2 - k) * quarter, quarter)]
        return remote(src, detour(k, n), detour_s.at[k - 1, n], detour_r.at[k - 1, n], near[k])

    def add_detour(n):
        for k in (1, 2):
            detour_copy(k, n).wait_recv()
        for k in (1, 2):
            for i in range(2):
                here = pair.at[last, n, pl.ds((k - 1) * half + i * quarter, quarter)]
                s = pl.ds(i * quarter, quarter)
                total = their_table[k - 1, 0, s, 0:1] * here[...].astype(f32)
                if i == k - 1:
                    total = total + their_table[k - 1, 1, s, 0:1] * detour(3 - k, n)[...].astype(f32)
                here[...] = total.astype(pair.dtype)

    def first_of(stage):
        return count - (count >> stage)

    def view(task, n):
        if task < 2:
            return pair.at[0, n, pl.ds(task * half, half)]
        if task == 3:
            return pair.at[2, n, pl.ds(0, half)]
        return pair.at[task - 1, n]

    def inbox(stage, task, m):
        if task < 2:
            return sum_in[stage - 1].at[task, m]
        if task == 3:
            return far_in[stage - 1].at[1, m, pl.ds(0, half)]
        return far_in[stage - 1].at[task - 2, m]

    def stage_copy(stage, task, m):
        return remote(
            view(task, first_of(stage - 1) + m), inbox(stage, task, m),
            stage_s.at[stage - 1, task, m], stage_r.at[stage - 1, task, m], mates[stage],
        )

    def send_stage(stage, task):
        for m in range(count >> stage):
            stage_copy(stage, task, m).start()

    def join_piece(stage, task, m):
        stage_copy(stage, task, m).wait()
        here = view(task, first_of(stage) + m)
        total = here[...].astype(f32) + inbox(stage, task, m)[...].astype(f32)
        here[...] = total.astype(pair.dtype)

    def join_stage(stage, task):
        for m in range(count >> stage):
            join_piece(stage, task, m)
        if stage < stages:
            send_stage(stage + 1, task)

    def meet(n):
        here = view(1, n)
        total = weight_of(0, 1) * here[...].astype(f32)
        for k in (1, 2):
            met_copy(k, n).wait_recv()
            total = total + met(k, n)[...].astype(f32)
        here[...] = total.astype(pair.dtype)
        for stage in range(1, stages + 1):
            if n < first_of(stage):
                stage_copy(stage, 1, n - first_of(stage - 1)).start()
                break
            join_piece(stage, 1, n - first_of(stage))

    def return_copies(b):
        done = pair.at[b, count - 1]
        if b == 2:
            return [remote(done.at[pl.ds(0, half)], home(3), ret_s.at[b], ret_r.at[b], near[3])]
        if b > 2:
            return [remote(done, home(b + 1), ret_s.at[b], ret_r.at[b], near[b + 1])]
        return [
            remote(
                done.at[pl.ds((k - 1) * half, half)], home(k),
                ret_s.at[k - 1], ret_r.at[k - 1], near[k],
            )
            for k in (1, 2)
        ]

    def finish(b):
        for stage in range(2, stages + 1):
            join_stage(stage, b + 1)
        for copy in return_copies(b):
            copy.start()

    def compute(b, first, hooks):
        for j in range(tiles):
            if first:
                if j == 0:
                    own_copy.wait()
                take_weights(j)
            s = pl.ds(j * tile, tile)
            gate_act = jnp.dot(blk[b], gate[:, s], preferred_element_type=f32)
            up_act = jnp.dot(blk[b], up[:, s], preferred_element_type=f32)
            hid[:, s] = (gate_act / (1.0 + jnp.exp(-gate_act)) * up_act).astype(hid.dtype)
            hooks("mid", j)
        for t in range(count):
            if first:
                take_weights(tiles + t)
            acc = jnp.dot(hid[...], down[:, columns(t)], preferred_element_type=f32).astype(part.dtype)
            for i in range(2):
                part[(core + i) % 2, t] = acc[:, i * cols : (i + 1) * cols]
            pair_copy(b, t).start()
            hooks("end", t)

    def first_hooks(phase, at):
        if phase == "end" and at < 2:
            pass_first(at)
        if (phase, at) == ("end", 1):
            send_second()

    def actions(step, phase, at):
        todo = []
        if (phase, at) == ("mid", 0):
            if step > 2:
                todo += [functools.partial(join_stage, 1, step - 1)]
            todo += [functools.partial(join_pair, step - 1, n) for n in range(count)]
            if step == 3:
                todo += [lambda k=k, n=n: detour_copy(k, n).start() for n in range(count) for k in (1, 2)]
            todo += [functools.partial(send_stage, 1, step if step > 1 else 0)]
        if (phase, at) == ("mid", 2) and step == 2:
            todo += [learn_routes]
        if (phase, at) == ("mid", 1) and step == 2:
            todo += [functools.partial(join_stage, stage, 0) for stage in range(2, stages + 1)]
        if (phase, at) == ("end", 0):
            if step == 1:
                todo += [functools.partial(join_stage, 1, 0)]
            if step == last - 1:
                todo += [pass_second]
        if (phase, at) == ("end", count - 2) and step < last - 1:
            todo += [functools.partial(pass_far, step + 2)]
        if (phase, at) == ("end", count - 1) and step > 2:
            todo += [functools.partial(finish, step - 2)]
        if step == last and phase == "end" and at > 0:
            todo += [functools.partial(hand_over, at - 1)]
        return todo

    compute(0, True, first_hooks)

    @pl.loop(1, experts)
    def _(step):
        for b in range(1, experts):
            @pl.when(step == b)
            def _():
                arrive(b)

        def hooks(phase, at):
            for b in range(1, experts):
                todo = actions(b, phase, at)
                if todo:
                    @pl.when(step == b)
                    def _():
                        for action in todo:
                            action()

        compute(step, False, hooks)

    hand_over(count - 1)
    join_stage(1, last)
    for n in range(count // 2):
        meet(n)
    finish(last - 1)
    for n in range(count // 2, count):
        meet(n)

    for k in range(1, experts):
        for h in range(2):
            for i in range(2):
                if (k, h) != (3, 0):
                    token_copy(k, h, i).wait_send()
                forward_copy(k, h, i).wait_send()
    for i in range(2):
        relay_copy(i).wait_send()
    for k in (1, 2):
        for copy in route_copies(k):
            copy.wait_send()
        for n in range(count):
            detour_copy(k, n).wait_send()
            met_copy(k, n).wait_send()
    for b in range(1, last):
        for copy in return_copies(b):
            copy.wait()
    for h in range(2):
        s = pl.ds(h * half, half)
        result = view(h, count - 1)[...].astype(f32)
        if h == 0:
            result = weight_of(0, 0) * result
        for k in range(4 if h else 1, experts):
            back = home(k)[...] if k < 4 else returned[k - 4, s]
            result = result + weight_of(k, h) * back.astype(f32)
        out_ref[s] = result.astype(out_ref.dtype)


def per_device(experts, groups, tokens, router_gates, routes, gate_proj, up_proj, down_proj):
    rows, width = tokens.shape
    hidden = gate_proj.shape[2]
    cols = width // groups
    count = groups // 2
    stages = groups.bit_length() - 2
    tile = 256 if hidden % 256 == 0 else 128
    bf16 = jnp.bfloat16
    dma = pltpu.SemaphoreType.DMA
    vmem = pl.BlockSpec(memory_space=pltpu.VMEM)
    hbm = pl.BlockSpec(memory_space=pl.ANY)
    half = rows // 2
    steps = hidden // tile + count
    far = experts - 2
    scratch = [
        pltpu.VMEM((width, hidden), bf16),
        pltpu.VMEM((width, hidden), bf16),
        pltpu.VMEM((hidden, width), bf16),
        pltpu.VMEM((experts, rows, width), bf16),
        pltpu.VMEM((rows, hidden), bf16),
        pltpu.VMEM((2, count, rows, cols), bf16),
        pltpu.VMEM((experts, count, rows, cols), bf16),
        pltpu.VMEM((max(experts - 4, 1), rows if experts > 4 else 16, cols), bf16),
        pltpu.VMEM((experts, rows, 128), jnp.float32),
        pltpu.VMEM((2,) + router_gates.shape[::-1], router_gates.dtype),
        pltpu.VMEM((2,) + routes.shape[::-1], routes.dtype),
        pltpu.VMEM((2, 2, half, 128), jnp.float32),
    ]
    scratch += [pltpu.VMEM((2, count >> s, half, cols), bf16) for s in range(1, stages + 1)]
    scratch += [pltpu.VMEM((far, count >> s, rows, cols), bf16) for s in range(1, stages + 1)]
    scratch += [dma((2, steps)), dma]
    scratch += [dma((experts, 2, 2))] * 4 + [dma((2,))] * 2
    scratch += [dma((experts, count))] * 2 + [dma((2, count))] * 2
    scratch += [dma((stages, 2 + far, count // 2))] * 2 + [dma((experts - 1,))] * 2
    scratch += [dma((2, count))] * 2 + [dma((2, 2))] * 2
    return pl.pallas_call(
        functools.partial(layer_kernel, experts, groups, tile),
        name="layer",
        out_shape=jax.ShapeDtypeStruct((rows, cols), bf16),
        in_specs=[hbm, vmem, vmem, hbm, hbm, hbm],
        out_specs=vmem,
        scratch_shapes=scratch,
        compiler_params=pltpu.CompilerParams(
            collective_id=0, has_side_effects=True, vmem_limit_bytes=VMEM_BYTES
        ),
    )(tokens, router_gates.T, routes.T, gate_proj[0], up_proj[0], down_proj[0])


def solution(mesh):
    in_specs = (
        P("expert", None),
        P("expert", None),
        P("expert", None),
        P("expert", None, "ffn"),
        P("expert", None, "ffn"),
        P("expert", "ffn", None),
    )
    body = functools.partial(per_device, mesh.shape["expert"], mesh.shape["ffn"])
    return jax.shard_map(
        body, mesh=mesh, in_specs=in_specs, out_specs=P("expert", "ffn"), check_vma=False
    )
```

```python
import functools

import jax
import jax.numpy as jnp
from jax import lax
from jax.experimental import pallas as pl
from jax.experimental.pallas import tpu as pltpu
from jax.sharding import PartitionSpec as P

MESH = pl.DeviceIdType.MESH
VMEM_BYTES = 67043328
AHEAD = 3


def flip(index, mask, size):
    result, bit = 0, 1
    while bit < size:
        digit = (index // bit) % 2
        result = result + bit * ((1 - digit) if mask & bit else digit)
        bit *= 2
    return result


def layer_kernel(
    experts, groups, tile,
    tokens_hbm, gates_ref, routes_ref, gate_hbm, up_hbm, down_hbm,
    out_ref,
    gate, up, down, blk, hid, part, pair, returned, table, their_gates, their_routes, their_table,
    *rest,
):
    stages = groups.bit_length() - 2
    sum_in, far_in, rest = rest[:stages], rest[stages : 2 * stages], rest[2 * stages :]
    (weight_sem, own_sem, tok_s, tok_r, fwd_s, fwd_r, relay_s, relay_r,
     pair_s, pair_r, met_s, met_r, stage_s, stage_r, ret_s, ret_r,
     detour_s, detour_r, route_s, route_r) = rest
    rows, width = blk.shape[1], blk.shape[2]
    hidden = gate.shape[1]
    half, quarter, piece = rows // 2, rows // 4, rows // 8
    cols = width // groups
    count = groups // 2
    tiles, out_tile = hidden // tile, 2 * cols
    last = experts - 1
    e, f = lax.axis_index("expert"), lax.axis_index("ffn")
    core = f % 2
    near = {k: (flip(e, k, experts), f) for k in range(1, experts)}
    mates = [(e, flip(f, 1 << s, groups)) for s in range(stages + 1)]
    far = list(range(3, experts))
    f32 = jnp.float32
    half_of_pair = (f // 2) % 2

    barrier = pltpu.get_barrier_semaphore()
    partners = list(near.values()) + mates
    for partner in partners:
        pl.semaphore_signal(barrier, inc=1, device_id=partner, device_id_type=MESH)

    own_copy = pltpu.make_async_copy(tokens_hbm, blk.at[0], own_sem)

    def columns(t):
        index = 0
        for s in range(1, stages + 1):
            digit = (f // (1 << s)) % 2
            index = index + (1 << (s - 1)) * (digit if (t >> (stages - s)) & 1 else 1 - digit)
        return pl.ds(pl.multiple_of(index * out_tile, out_tile), out_tile)

    def weight_group(i):
        if i < tiles:
            s = pl.ds(i * tile, tile)
            return [
                pltpu.make_async_copy(gate_hbm.at[:, s], gate.at[:, s], weight_sem.at[0, i]),
                pltpu.make_async_copy(up_hbm.at[:, s], up.at[:, s], weight_sem.at[1, i]),
            ]
        s = columns(i - tiles)
        return [pltpu.make_async_copy(down_hbm.at[:, s], down.at[:, s], weight_sem.at[0, i])]

    def start_weights(i):
        if i < tiles + count:
            for copy in weight_group(i):
                copy.start()

    def take_weights(i):
        for copy in weight_group(i):
            copy.wait()
        start_weights(i + AHEAD)

    own_copy.start()
    for i in range(AHEAD):
        start_weights(i)

    def place(k, h):
        return (last if h else 1, (k - 1) * half) if k < 3 else (k - 1, h * half)

    def remote(src, dst, ss, rs, device):
        return pltpu.make_async_remote_copy(
            src_ref=src, dst_ref=dst, send_sem=ss, recv_sem=rs, device_id=device, device_id_type=MESH
        )

    def which(k, h, i):
        if (k, h) == (3, 1):
            return 1 - half_of_pair if i else half_of_pair
        return i

    def spot(k, h, i):
        b, row = place(k, h)
        return blk.at[b, pl.ds(pl.multiple_of(row + core * quarter + which(k, h, i) * piece, piece), piece)]

    def token_copy(k, h, i):
        if (k, h, i) == (3, 1, 1):
            here = spot(3, 1, 0)
            return remote(here, here, tok_s.at[k, h, i], tok_r.at[k, h, i], mates[1])
        row = pl.multiple_of(h * half + core * quarter + which(k, h, i) * piece, piece)
        return remote(
            tokens_hbm.at[pl.ds(row, piece)], spot(k, h, i), tok_s.at[k, h, i], tok_r.at[k, h, i], near[k]
        )

    def forward_copy(k, h, i):
        return remote(spot(k, h, i), spot(k, h, i), fwd_s.at[k, h, i], fwd_r.at[k, h, i], mates[0])

    def weight_rows(gates, routes, name):
        total = jnp.zeros((1, rows), f32)
        for t in range(routes.shape[0]):
            total = total + jnp.where(routes[t : t + 1, :] == name, gates[t : t + 1, :], 0.0)
        return jnp.broadcast_to(total, (128, rows)).T

    def route_copies(k):
        return [
            remote(ref, theirs.at[k - 1], route_s.at[i, k - 1], route_r.at[i, k - 1], near[k])
            for i, (ref, theirs) in enumerate([(gates_ref, their_gates), (routes_ref, their_routes)])
        ]

    def relay_copy(i):
        return remote(spot(2 - i, 0, i), spot(3, 0, i), relay_s.at[i], relay_r.at[i], near[1 + i])

    for k in range(experts):
        table[k] = weight_rows(gates_ref[...], routes_ref[...], flip(e, k, experts))
    pl.semaphore_wait(barrier, len(partners))
    for i in range(2):
        for k in (1, 2):
            token_copy(k, 0, i).start()
    for k in (1, 2):
        for copy in route_copies(k):
            copy.start()
    for k in far:
        for h in range(1 if k == 3 else 0, 2):
            for i in range(2):
                if (k, h, i) != (3, 1, 1):
                    token_copy(k, h, i).start()

    def share():
        token_copy(3, 1, 0).wait_recv()
        forward_copy(3, 1, 0).start()
        token_copy(3, 1, 1).start()

    def pass_first(i):
        for k in (1, 2):
            token_copy(k, 0, i).wait_recv()
            forward_copy(k, 0, i).start()
        relay_copy(i).start()

    def free_first():
        for i in range(2):
            relay_copy(i).wait_send()
            for k in (1, 2):
                forward_copy(k, 0, i).wait_send()

    def send_second():
        for i in range(2):
            for k in (1, 2):
                token_copy(k, 1, i).start()

    def pass_second():
        for i in range(2):
            for k in (1, 2):
                token_copy(k, 1, i).wait_recv()
                forward_copy(k, 1, i).start()

    def pass_far(k):
        for h in (1, 0):
            for i in range(2):
                if (k, h, i) == (3, 1, 0):
                    continue
                if k == 3 and h == 0:
                    relay_copy(i).wait_recv()
                else:
                    token_copy(k, h, i).wait_recv()
                forward_copy(k, h, i).start()

    def arrive(b):
        if b in (1, last):
            pairs = [(1, b // last), (2, b // last)]
        else:
            pairs = [(b + 1, 0), (b + 1, 1)]
        for k, h in pairs:
            for i in range(2):
                forward_copy(k, h, i).wait_recv()

    def pair_copy(b, n):
        return remote(part.at[1, n], pair.at[b, n], pair_s.at[b, n], pair_r.at[b, n], mates[0])

    def join_pair(b, n):
        pair_copy(b, n).wait()
        pair[b, n] = (part[0, n].astype(f32) + pair[b, n].astype(f32)).astype(pair.dtype)

    def met_copy(k, h, n):
        b, row = place(k, h)
        return remote(
            pair.at[b, n, pl.ds(row, half)], met(k, h, n),
            met_s.at[k - 1, h, n], met_r.at[k - 1, h, n], near[k],
        )

    def hand_over(n):
        join_pair(last, n)
        add_detour(n)
        for k in (1, 2):
            met_copy(k, 1, n).start()

    def weight_of(k, h):
        return table[k, pl.ds(h * half, half), 0:1]

    def learn_routes():
        for k in (1, 2):
            for copy in route_copies(k):
                copy.wait_recv()
            for i, name in enumerate([e, near[3 - k][0]]):
                their_table[k - 1, i] = weight_rows(their_gates[k - 1], their_routes[k - 1], name)[half:]

    def met(k, h, n):
        return blk.at[h, pl.ds((k - 1) * half, half), pl.ds(n * cols, cols)]

    def detour(k, n):
        return blk.at[0, pl.ds((k - 1) * quarter, quarter), pl.ds(width // 2 + n * cols, cols)]

    def home(k):
        if k < 4:
            return blk.at[0, pl.ds(half, half), pl.ds(width // 2, cols)]
        return returned.at[k - 4]

    def detour_copy(k, n):
        src = pair.at[2, n, pl.ds(half + (2 - k) * quarter, quarter)]
        return remote(src, detour(k, n), detour_s.at[k - 1, n], detour_r.at[k - 1, n], near[k])

    def add_detour(n):
        for k in (1, 2):
            detour_copy(k, n).wait_recv()
        for k in (1, 2):
            for i in range(2):
                here = pair.at[last, n, pl.ds((k - 1) * half + i * quarter, quarter)]
                s = pl.ds(i * quarter, quarter)
                total = their_table[k - 1, 0, s, 0:1] * here[...].astype(f32)
                if i == k - 1:
                    total = total + their_table[k - 1, 1, s, 0:1] * detour(3 - k, n)[...].astype(f32)
                here[...] = total.astype(pair.dtype)

    def first_of(stage):
        return count - (count >> stage)

    def view(task, n):
        if task < 2:
            return pair.at[0, n, pl.ds(task * half, half)]
        if task == 3:
            return pair.at[2, n, pl.ds(0, half)]
        return pair.at[task - 1, n]

    def inbox(stage, task, m):
        if task < 2:
            return sum_in[stage - 1].at[task, m]
        if task == 3:
            return far_in[stage - 1].at[1, m, pl.ds(0, half)]
        return far_in[stage - 1].at[task - 2, m]

    def stage_copy(stage, task, m):
        return remote(
            view(task, first_of(stage - 1) + m), inbox(stage, task, m),
            stage_s.at[stage - 1, task, m], stage_r.at[stage - 1, task, m], mates[stage],
        )

    def send_stage(stage, task):
        for m in range(count >> stage):
            stage_copy(stage, task, m).start()

    def join_piece(stage, task, m):
        stage_copy(stage, task, m).wait()
        here = view(task, first_of(stage) + m)
        total = here[...].astype(f32) + inbox(stage, task, m)[...].astype(f32)
        here[...] = total.astype(pair.dtype)

    def join_stage(stage, task):
        for m in range(count >> stage):
            join_piece(stage, task, m)
        if stage < stages:
            send_stage(stage + 1, task)

    def meet(h, n):
        here = view(h, n)
        total = weight_of(0, h) * here[...].astype(f32)
        for k in (1, 2):
            met_copy(k, h, n).wait_recv()
            got = met(k, h, n)[...].astype(f32)
            total = total + (got if h else weight_of(k, h) * got)
        here[...] = total.astype(pair.dtype)
        if n < first_of(1):
            stage_copy(1, h, n).start()

    def settle(n):
        for stage in range(1, stages + 1):
            if n < first_of(stage):
                stage_copy(stage, 1, n - first_of(stage - 1)).start()
                break
            join_piece(stage, 1, n - first_of(stage))

    def return_copies(b):
        done = pair.at[b, count - 1]
        if b == 2:
            return [remote(done.at[pl.ds(0, half)], home(3), ret_s.at[b], ret_r.at[b], near[3])]
        return [remote(done, home(b + 1), ret_s.at[b], ret_r.at[b], near[b + 1])]

    def finish(b):
        for stage in range(2, stages + 1):
            join_stage(stage, b + 1)
        for copy in return_copies(b):
            copy.start()

    def compute(b, first, hooks):
        for j in range(tiles):
            if first:
                if j == 0:
                    own_copy.wait()
                take_weights(j)
            s = pl.ds(j * tile, tile)
            gate_act = jnp.dot(blk[b], gate[:, s], preferred_element_type=f32)
            up_act = jnp.dot(blk[b], up[:, s], preferred_element_type=f32)
            hid[:, s] = (gate_act / (1.0 + jnp.exp(-gate_act)) * up_act).astype(hid.dtype)
            hooks("mid", j)
        for t in range(count):
            if first:
                take_weights(tiles + t)
            acc = jnp.dot(hid[...], down[:, columns(t)], preferred_element_type=f32).astype(part.dtype)
            for i in range(2):
                part[(core + i) % 2, t] = acc[:, i * cols : (i + 1) * cols]
            pair_copy(b, t).start()
            hooks("end", t)

    def first_hooks(phase, at):
        if phase == "end" and at < 2:
            pass_first(at)
        if (phase, at) == ("end", 1):
            send_second()

    def actions(step, phase, at):
        todo = []
        if (phase, at) == ("mid", 0):
            if step == 1:
                todo += [share]
            if step == 3:
                todo += [functools.partial(meet, 0, n) for n in range(count // 2, count)]
            if step > 3:
                todo += [functools.partial(join_stage, 1, step - 1)]
            todo += [functools.partial(join_pair, step - 1, n) for n in range(count)]
            if step == 2:
                todo += [free_first]
                todo += [lambda k=k, n=n: met_copy(k, 0, n).start() for n in range(count) for k in (1, 2)]
            if step == 3:
                todo += [lambda k=k, n=n: detour_copy(k, n).start() for n in range(count) for k in (1, 2)]
            if step > 2:
                todo += [functools.partial(send_stage, 1, step)]
        if (phase, at) == ("end", 1) and step == 2:
            todo += [functools.partial(meet, 0, n) for n in range(count // 2)]
        if (phase, at) == ("mid", 2) and step == 3:
            todo += [functools.partial(join_stage, 1, 0)]
        if (phase, at) == ("mid", 2) and step == 2:
            todo += [learn_routes]
        if (phase, at) == ("end", 0):
            if step == last - 1:
                todo += [pass_second]
            if step < last - 1:
                todo += [functools.partial(pass_far, step + 2)]
        if (phase, at) == ("end", count - 1):
            if 3 < step < last:
                todo += [functools.partial(finish, step - 2)]
        if step == last and phase == "end" and at > 0:
            todo += [functools.partial(hand_over, at - 1)]
            if at == count - 2:
                todo += [functools.partial(join_stage, 1, last)]
        return todo

    compute(0, True, first_hooks)

    @pl.loop(1, experts)
    def _(step):
        for b in range(1, experts):
            @pl.when(step == b)
            def _():
                arrive(b)

        def hooks(phase, at):
            for b in range(1, experts):
                todo = actions(b, phase, at)
                if todo:
                    @pl.when(step == b)
                    def _():
                        for action in todo:
                            action()

        compute(step, False, hooks)

    hand_over(count - 1)
    if last > 3:
        finish(last - 2)
    for n in range(count - 1):
        meet(1, n)
        if n >= first_of(1):
            settle(n)
    for stage in range(2, stages + 1):
        join_stage(stage, 0)
    finish(last - 1)
    meet(1, count - 1)
    settle(count - 1)

    for k in range(1, experts):
        for h in range(2):
            for i in range(2):
                if (k, h) != (3, 0):
                    token_copy(k, h, i).wait_send()
                if k > 2 or h:
                    forward_copy(k, h, i).wait_send()
    for k in (1, 2):
        for copy in route_copies(k):
            copy.wait_send()
        for n in range(count):
            detour_copy(k, n).wait_send()
            for h in range(2):
                met_copy(k, h, n).wait_send()
    for b in range(2, last):
        for copy in return_copies(b):
            copy.wait()
    for h in range(2):
        s = pl.ds(h * half, half)
        result = view(h, count - 1)[...].astype(f32)
        for k in range(4 if h else 3, experts):
            back = home(k)[...] if k < 4 else returned[k - 4, s]
            result = result + weight_of(k, h) * back.astype(f32)
        out_ref[s] = result.astype(out_ref.dtype)


def per_device(experts, groups, tokens, router_gates, routes, gate_proj, up_proj, down_proj):
    rows, width = tokens.shape
    hidden = gate_proj.shape[2]
    cols = width // groups
    count = groups // 2
    stages = groups.bit_length() - 2
    tile = 256 if hidden % 256 == 0 else 128
    bf16 = jnp.bfloat16
    dma = pltpu.SemaphoreType.DMA
    vmem = pl.BlockSpec(memory_space=pltpu.VMEM)
    hbm = pl.BlockSpec(memory_space=pl.ANY)
    half = rows // 2
    steps = hidden // tile + count
    far = experts - 2
    scratch = [
        pltpu.VMEM((width, hidden), bf16),
        pltpu.VMEM((width, hidden), bf16),
        pltpu.VMEM((hidden, width), bf16),
        pltpu.VMEM((experts, rows, width), bf16),
        pltpu.VMEM((rows, hidden), bf16),
        pltpu.VMEM((2, count, rows, cols), bf16),
        pltpu.VMEM((experts, count, rows, cols), bf16),
        pltpu.VMEM((max(experts - 4, 1), rows if experts > 4 else 16, cols), bf16),
        pltpu.VMEM((experts, rows, 128), jnp.float32),
        pltpu.VMEM((2,) + router_gates.shape[::-1], router_gates.dtype),
        pltpu.VMEM((2,) + routes.shape[::-1], routes.dtype),
        pltpu.VMEM((2, 2, half, 128), jnp.float32),
    ]
    scratch += [pltpu.VMEM((2, count >> s, half, cols), bf16) for s in range(1, stages + 1)]
    scratch += [pltpu.VMEM((far, count >> s, rows, cols), bf16) for s in range(1, stages + 1)]
    scratch += [dma((2, steps)), dma]
    scratch += [dma((experts, 2, 2))] * 4 + [dma((2,))] * 2
    scratch += [dma((experts, count))] * 2 + [dma((2, 2, count))] * 2
    scratch += [dma((stages, 2 + far, count // 2))] * 2 + [dma((experts - 1,))] * 2
    scratch += [dma((2, count))] * 2 + [dma((2, 2))] * 2
    return pl.pallas_call(
        functools.partial(layer_kernel, experts, groups, tile),
        name="layer",
        out_shape=jax.ShapeDtypeStruct((rows, cols), bf16),
        in_specs=[hbm, vmem, vmem, hbm, hbm, hbm],
        out_specs=vmem,
        scratch_shapes=scratch,
        compiler_params=pltpu.CompilerParams(
            collective_id=0, has_side_effects=True, vmem_limit_bytes=VMEM_BYTES
        ),
    )(tokens, router_gates.T, routes.T, gate_proj[0], up_proj[0], down_proj[0])


def solution(mesh):
    in_specs = (
        P("expert", None),
        P("expert", None),
        P("expert", None),
        P("expert", None, "ffn"),
        P("expert", None, "ffn"),
        P("expert", "ffn", None),
    )
    body = functools.partial(per_device, mesh.shape["expert"], mesh.shape["ffn"])
    return jax.shard_map(
        body, mesh=mesh, in_specs=in_specs, out_specs=P("expert", "ffn"), check_vma=False
    )
```
